32 devices in a mesh: row: 4 (over z), col: 2 (over x), depth: 4 (over y, core).
Axes of the slice: x: 2, y: 2, z: 4, core: 2. Of those that a mesh axis runs over, the one named last changes fastest.
Arguments:
- eri_tiles: bfloat16 [48, 64, 128, 128], P('row', ('col', 'depth')), may hold values from -0.0625 to 0.0625
- screen: int32 [48, 64], P('row', ('col', 'depth')), may hold values from 0 to 1, as said below
- density_bra: bfloat16 [6144, 256], P('row', 'col'), may hold values from -6 to 6
- density_ket: bfloat16 [8192, 256], P(('col', 'depth'), 'row'), may hold values from -6 to 6
Outputs:
- coulomb_bra: float32 [6144, 256], P('row', 'col')
- coulomb_ket: float32 [8192, 256], P(('col', 'depth'), 'row')
The draws below stay inside these ranges and needn't reach their ends.
Inputs may be any that keep to these rules, and one draw needn't show every extreme that they name: `screen`: in each device's block of 12 x 8 tiles (aligned blocks), between 16 and 64 tiles are significant; some block has exactly 64.
All inputs are finite; a program needn't handle non-finite values.
Results may differ from the reference program's by a relative error of at most 0.005.
Values may be sent and summed in bfloat16 or wider, within the bound.
A program may use at most 64 MiB of HBM per device.

```python
import jax
import jax.numpy as jnp
from jax import lax

PAIR = 128
DENS = 256
A_DEV = 12
B_DEV = 8
NA = 48
NB = 64
CAP = 64


def draw_screen(key, part):
    blocks_r = NA // A_DEV
    blocks_c = NB // B_DEV
    tiles_dev = A_DEV * B_DEV
    devices_all = blocks_r * blocks_c
    lowest = max(1, CAP // 4)
    key_count, key_pick, key_perm = jax.random.split(jax.random.fold_in(key, 11), 3)
    counts = jax.random.randint(key_count, (devices_all,), lowest, CAP + 1)
    busiest = jax.random.randint(key_pick, (), 0, devices_all)
    counts = jnp.where(jnp.arange(devices_all) == busiest, CAP, counts)
    sub_keys = jax.random.split(key_perm, devices_all)

    def permute_one(subkey):
        return jax.random.permutation(subkey, tiles_dev)
    ranking = jax.vmap(permute_one)(sub_keys)
    significant = (ranking < counts[:, None]).astype(jnp.int32)
    return significant.reshape(blocks_r, blocks_c, A_DEV, B_DEV).transpose(0, 2, 1, 3).reshape(NA, NB)


def block_levels(rng, shape, shards, smallest, largest):
    def one(position, parts):
        steps = jax.random.uniform(jax.random.fold_in(jax.random.fold_in(rng, 6), position), (parts,), jnp.float32, smallest / len(shards), largest / len(shards))
        return jnp.repeat(jnp.exp(steps), shape[position] // parts).reshape((-1,) + (1,) * (len(shape) - position - 1))

    gain = one(*shards[0])
    for cut in shards[1:]:
        gain = gain * one(*cut)
    return gain


def noise(own_key, shape, scale, reach, cuts=(), kind=jnp.bfloat16):
    array = jax.random.normal(own_key, shape, jnp.float32) * scale
    if len(cuts) > 0:
        array = block_levels(own_key, shape, cuts, -0.22, 0.18) * array
    return jnp.clip(array, min=-reach, max=reach).astype(kind)


def setup_inputs(seed: int = 0) -> dict:
    arg_keys = jax.random.split(jax.random.key(seed), 5)
    return {
        "eri_tiles": noise(arg_keys[0], (NA, NB, PAIR, PAIR), (PAIR * (NA + NB) // 2) ** -0.5, 0.0625, ((0, 4), (1, 8))),
        "screen": draw_screen(jax.random.fold_in(arg_keys[4], 71), 0),
        "density_bra": noise(arg_keys[2], (NA * PAIR, DENS), 1.0, 6.0, ((0, 4), (1, 2))),
        "density_ket": noise(arg_keys[3], (NB * PAIR, DENS), 1.0, 6.0, ((0, 8), (1, 4))),
    }


def reference(eri_tiles, screen, density_bra, density_ket):
    keep = screen.astype(jnp.float32)
    ket_rows = density_ket.astype(jnp.float32).reshape(NB, PAIR, DENS)
    bra_rows = density_bra.astype(jnp.float32).reshape(NA, PAIR, DENS)

    def advance(carry, inputs):
        tiles, weights, bra_block = inputs
        masked = tiles.astype(jnp.float32) * weights[:, None, None]
        row_out = jnp.einsum('bij,bjr->ir', masked, ket_rows)
        carry = carry + jnp.einsum('bij,ir->bjr', masked, bra_block)
        return carry, row_out

    start_sum = jnp.zeros((NB, PAIR, DENS), jnp.float32)
    ket_total, bra_out = lax.scan(advance, start_sum, (eri_tiles, keep, bra_rows))
    return bra_out.reshape(NA * PAIR, DENS), ket_total.reshape(NB * PAIR, DENS)
```

```python
import functools

import jax
import jax.numpy as jnp
from jax import lax
from jax.experimental import pallas as pl
from jax.experimental.pallas import tpu as pltpu
from jax.sharding import PartitionSpec as P

MESH = pl.DeviceIdType.MESH
F32 = jnp.float32


def kernel(
    sizes, eri, scr, dbra, dket, out_b, out_k,
    traw, tmat, kbuf, bbuf, kpart, down_rx, up_rx, bp, d1_rx, x_rx, y_rx, fin,
    local_sem, ks_send, ks_recv, b_send, b_recv, kr_send, kr_recv, bp_send, bp_recv,
):
    R, C, Dp = sizes
    per = R // C
    G = Dp // 2
    r, c, d = lax.axis_index("row"), lax.axis_index("col"), lax.axis_index("depth")
    h = d % 2
    g = d // 2
    sib = {"depth": d + 1 - 2 * h}
    up, down = {"row": r + 1}, {"row": r - 1}
    A, B, PS = eri.shape[0], eri.shape[1], eri.shape[2]
    rows, cols = tmat.shape
    dk = kbuf.shape[1]
    db = bbuf.shape[3]
    pending = []

    def send(src, dst, ssem, rsem, dev, cond=None):
        def make():
            return pltpu.make_async_remote_copy(
                src_ref=src, dst_ref=dst, send_sem=ssem, recv_sem=rsem,
                device_id=dev, device_id_type=MESH)

        def start():
            make().start()

        if cond is None:
            start()
        else:
            pl.when(cond)(start)
        pending.append((cond, lambda: make().wait_send()))

    def recv(dst, ssem, rsem, cond=None):
        def go():
            pltpu.make_async_remote_copy(
                src_ref=dst, dst_ref=dst, send_sem=ssem, recv_sem=rsem,
                device_id=sib, device_id_type=MESH).wait_recv()
        if cond is None:
            go()
        else:
            pl.when(cond)(go)

    half = rows // 2
    loads = [
        pltpu.make_async_copy(dket, kbuf.at[r], local_sem.at[0]),
        pltpu.make_async_copy(dbra.at[pl.ds(0, half)], bbuf.at[c, 0], local_sem.at[1]),
        pltpu.make_async_copy(dbra.at[pl.ds(half, half)], bbuf.at[c, 1], local_sem.at[2]),
        pltpu.make_async_copy(eri, traw, local_sem.at[3]),
    ]
    for one in loads:
        one.start()

    bar = pltpu.get_barrier_semaphore()

    def hello(dev):
        pl.semaphore_signal(bar, inc=1, device_id=dev, device_id_type=MESH)

    pl.when(r > 0)(lambda: hello(down))
    pl.when(r < R - 1)(lambda: hello(up))
    for o in range(1, C):
        hello({"col": (c + o) % C})
    hello(sib)
    for o in range(1, G):
        hello({"depth": (d + 2 * o) % Dp})
    peers = C + G - 1 + jnp.where(r > 0, 1, 0) + jnp.where(r < R - 1, 1, 0)
    pl.semaphore_wait(bar, peers)

    loads[0].wait()
    send(kbuf.at[r], kbuf.at[r], ks_send.at[r, 0], ks_recv.at[r], down, r > 0)
    send(kbuf.at[r], kbuf.at[r], ks_send.at[r, 1], ks_recv.at[r], up, r < R - 1)
    loads[1].wait()
    loads[2].wait()
    for o in range(1, C):
        send(bbuf.at[c, h], bbuf.at[c, h], b_send.at[o], b_recv.at[0, c], {"col": (c + o) % C})
    loads[3].wait()

    for a in range(A):
        for b in range(B):
            keep = scr[b, a] > 0
            tile = traw[a, b]
            tmat[a * PS:(a + 1) * PS, b * PS:(b + 1) * PS] = jnp.where(keep, tile, jnp.zeros_like(tile))

    def ket_block(cb):
        x = bbuf[cb].reshape(rows, db)
        res = lax.dot_general(x, tmat[...], (((0,), (0,)), ((), ())), preferred_element_type=F32)
        for j in range(per):
            kpart[cb * per + j] = res[j * dk:(j + 1) * dk]

    def ket_ends(cb):
        for j in range(per):
            t = cb * per + j
            send(kpart.at[t], down_rx.at[t], kr_send.at[0, t], kr_recv.at[0, t], down,
                 (r == R - 1) & (t < r))
        for j in reversed(range(per)):
            t = cb * per + j
            send(kpart.at[t], up_rx.at[t], kr_send.at[1, t], kr_recv.at[1, t], up,
                 (r == 0) & (t > r))

    def ket_forward(k):
        def go_down():
            recv(down_rx.at[k], kr_send.at[0, k], kr_recv.at[0, k])
            kpart[k] = kpart[k] + down_rx[k]
        cond = (r < R - 1) & (k < r)
        pl.when(cond)(go_down)
        send(kpart.at[k], down_rx.at[k], kr_send.at[0, k], kr_recv.at[0, k], down, cond)
        t = R - 1 - k

        def go_up():
            recv(up_rx.at[t], kr_send.at[1, t], kr_recv.at[1, t])
            kpart[t] = kpart[t] + up_rx[t]
        cond = (r > 0) & (t > r)
        pl.when(cond)(go_up)
        send(kpart.at[t], up_rx.at[t], kr_send.at[1, t], kr_recv.at[1, t], up, cond)

    def ket_final():
        out_k[...] = kpart[r]

        def from_up():
            recv(down_rx.at[r], kr_send.at[0, r], kr_recv.at[0, r])
            out_k[...] += down_rx[r]

        def from_down():
            recv(up_rx.at[r], kr_send.at[1, r], kr_recv.at[1, r])
            out_k[...] += up_rx[r]
        pl.when(r < R - 1)(from_up)
        pl.when(r > 0)(from_down)

    near = jnp.minimum(r, R - 1 - r)

    def slot(i):
        k = (i + 1) // 2
        inner = r - k if i % 2 == 1 else r + k
        outer = jnp.where(r > R - 1 - r, r - (i - near), r + (i - near))
        return jnp.where(i <= 2 * near, inner, outer)

    order = [slot(i) for i in range(R)]

    def bra_a(i):
        s = order[i]
        if i > 0:
            recv(kbuf.at[s], ks_send.at[s, 0], ks_recv.at[s])
            send(kbuf.at[s], kbuf.at[s], ks_send.at[s, 0], ks_recv.at[s], down, (s > r) & (r > 0))
            send(kbuf.at[s], kbuf.at[s], ks_send.at[s, 1], ks_recv.at[s], up, (s < r) & (r < R - 1))

    def bra_dot(i):
        s = order[i]
        res = lax.dot_general(kbuf[s], tmat[...], (((1,), (1,)), ((), ())), preferred_element_type=F32)
        bp[s, 0] = res[:, :half]
        bp[s, 1] = res[:, half:]
        send(bp.at[s, 1 - h], d1_rx.at[s], bp_send.at[0, s], bp_recv.at[0, s], sib)

    def bra_b(i):
        s = order[i]
        cs, j = s // per, s % per
        recv(d1_rx.at[s], bp_send.at[0, s], bp_recv.at[0, s])
        bp[s, h] = bp[s, h] + d1_rx[s]
        send(bp.at[s, h], x_rx.at[c, j], bp_send.at[1, s], bp_recv.at[1, c * per + j], {"col": cs}, cs != c)

    def bra_c(i):
        s = order[i]
        cs, j = s // per, s % per

        def go():
            total = bp[s, h]
            for o in range(1, C):
                p = (c + o) % C
                recv(x_rx.at[p, j], bp_send.at[1, s], bp_recv.at[1, p * per + j])
                total = total + x_rx[p, j]
            y_rx[j, g] = total
        pl.when(cs == c)(go)
        for o in range(1, G):
            send(y_rx.at[j, g], y_rx.at[j, g], bp_send.at[1 + o, s], bp_recv.at[2, j * G + g],
                 {"depth": (d + 2 * o) % Dp}, cs == c)

    def bra_d(i):
        s = order[i]
        cs, j = s // per, s % per

        def go():
            for o in range(1, G):
                q = (g + o) % G
                recv(y_rx.at[j, q], bp_send.at[2, s], bp_recv.at[2, j * G + q])
            total = y_rx[j, 0]
            for q in range(1, G):
                total = total + y_rx[j, q]
            fin[j, h] = total
        pl.when(cs == c)(go)
        send(fin.at[j, h], fin.at[j, h], bp_send.at[G + 1, s], bp_recv.at[3, j], sib, cs == c)

    def bra_e():
        for j in range(per):
            recv(fin.at[j, 1 - h], bp_send.at[G + 1, 0], bp_recv.at[3, j])
            out_b[j * dk:(j + 1) * dk, :half] = fin[j, 0]
            out_b[j * dk:(j + 1) * dk, half:] = fin[j, 1]

    ket_block(c)
    ket_ends(c)
    bra_dot(0)
    others = [(c + o) % C for o in range(1, C)]
    bra_a(1)
    for p in others:
        recv(bbuf.at[p, h], b_send.at[0], b_recv.at[0, p])
        send(bbuf.at[p, h], bbuf.at[p, h], b_send.at[C + p], b_recv.at[1, p], sib)
    bra_b(0)
    bra_dot(1)
    for i in range(2, R):
        bra_a(i)
        if i == 2:
            for p in others:
                recv(bbuf.at[p, 1 - h], b_send.at[0], b_recv.at[1, p])
                ket_block(p)
                ket_ends(p)
        bra_b(i - 1)
        bra_dot(i)
        if i == 2:
            bra_c(0)
            ket_forward(0)
    bra_b(R - 1)
    for i in range(1, R):
        if i < R - 1:
            ket_forward(i)
        bra_c(i)
        bra_d(i - 1)
    bra_d(R - 1)
    bra_e()
    ket_final()

    for cond, wait in pending:
        if cond is None:
            wait()
        else:
            pl.when(cond)(wait)


def body(sizes, eri_tiles, screen, density_bra, density_ket):
    R, C, Dp = sizes
    A, B, PS, _ = eri_tiles.shape
    rows, cols = A * PS, B * PS
    db, dk = density_bra.shape[1], density_ket.shape[1]
    per, G, half = R // C, Dp // 2, rows // 2
    DMA = pltpu.SemaphoreType.DMA
    anyspec = pl.BlockSpec(memory_space=pl.ANY)
    vm = pl.BlockSpec(memory_space=pltpu.VMEM)
    out_b, out_k = pl.pallas_call(
        functools.partial(kernel, sizes),
        out_shape=(jax.ShapeDtypeStruct((db, rows), F32), jax.ShapeDtypeStruct((dk, cols), F32)),
        in_specs=[anyspec, pl.BlockSpec(memory_space=pltpu.SMEM), anyspec, anyspec],
        out_specs=(vm, vm),
        scratch_shapes=[
            pltpu.VMEM((A, B, PS, PS), jnp.bfloat16),
            pltpu.VMEM((rows, cols), jnp.bfloat16),
            pltpu.VMEM((R, dk, cols), jnp.bfloat16),
            pltpu.VMEM((C, 2, half, db), jnp.bfloat16),
            pltpu.VMEM((R, dk, cols), F32),
            pltpu.VMEM((R, dk, cols), F32),
            pltpu.VMEM((R, dk, cols), F32),
            pltpu.VMEM((R, 2, dk, half), F32),
            pltpu.VMEM((R, dk, half), F32),
            pltpu.VMEM((C, per, dk, half), F32),
            pltpu.VMEM((per, G, dk, half), F32),
            pltpu.VMEM((per, 2, dk, half), F32),
            DMA((4,)),
            DMA((R, 2)), DMA((R,)),
            DMA((2 * C,)), DMA((2, C)),
            DMA((2, R)), DMA((2, R)),
            DMA((G + 2, R)), DMA((4, max(R, per * G))),
        ],
        compiler_params=pltpu.CompilerParams(
            collective_id=0, has_side_effects=True, vmem_limit_bytes=56 * 1024 * 1024),
    )(eri_tiles, screen.T, density_bra, density_ket.T)
    return out_b.T, out_k.T


def solution(mesh):
    sizes = (mesh.shape["row"], mesh.shape["col"], mesh.shape["depth"])
    return jax.shard_map(
        functools.partial(body, sizes),
        mesh=mesh,
        in_specs=(
            P("row", ("col", "depth"), None, None),
            P("row", ("col", "depth")),
            P("row", "col"),
            P(("col", "depth"), "row"),
        ),
        out_specs=(P("row", "col"), P(("col", "depth"), "row")),
        check_vma=False,
    )
```

```python
import functools

import jax
import jax.numpy as jnp
from jax import lax
from jax.experimental import pallas as pl
from jax.experimental.pallas import tpu as pltpu
from jax.sharding import PartitionSpec as P

MESH = pl.DeviceIdType.MESH
F32 = jnp.float32


def kernel(
    sizes, eri, scr, dbra, dket, out_b, out_k,
    traw, tmat, kbuf, bbuf, kpart, k_rx, bp, d1_rx, x_rx, y_rx, fin,
    local_sem, ks_send, ks_recv, b_send, b_recv, kr_send, kr_recv, bp_send, bp_recv,
):
    R, C, Dp = sizes
    per = R // C
    G = Dp // 2
    r, c, d = lax.axis_index("row"), lax.axis_index("col"), lax.axis_index("depth")
    h = d % 2
    g = d // 2
    sib = {"depth": d + 1 - 2 * h}
    up, down = {"row": r + 1}, {"row": r - 1}
    A, B, PS = eri.shape[0], eri.shape[1], eri.shape[2]
    rows, cols = tmat.shape
    dk = kbuf.shape[2]
    H = kbuf.shape[1]
    part = cols // H
    db = bbuf.shape[3]
    pending = []

    def send(src, dst, ssem, rsem, dev, cond=None):
        def make():
            return pltpu.make_async_remote_copy(
                src_ref=src, dst_ref=dst, send_sem=ssem, recv_sem=rsem,
                device_id=dev, device_id_type=MESH)

        def start():
            make().start()

        if cond is None:
            start()
        else:
            pl.when(cond)(start)
        pending.append((cond, lambda: make().wait_send()))

    def recv(dst, ssem, rsem, cond=None):
        def go():
            pltpu.make_async_remote_copy(
                src_ref=dst, dst_ref=dst, send_sem=ssem, recv_sem=rsem,
                device_id=sib, device_id_type=MESH).wait_recv()
        if cond is None:
            go()
        else:
            pl.when(cond)(go)

    half = rows // 2
    loads = [
        pltpu.make_async_copy(dbra.at[pl.ds(0, half)], bbuf.at[c, 0], local_sem.at[0]),
        pltpu.make_async_copy(dbra.at[pl.ds(half, half)], bbuf.at[c, 1], local_sem.at[1]),
        pltpu.make_async_copy(eri, traw, local_sem.at[2]),
    ]
    kloads = [
        pltpu.make_async_copy(dket.at[:, pl.ds(u * part, part)], kbuf.at[r, u], local_sem.at[3 + u])
        for u in range(H)
    ]
    for one in kloads:
        one.start()
    for one in loads:
        one.start()

    bar = pltpu.get_barrier_semaphore()

    def hello(dev):
        pl.semaphore_signal(bar, inc=1, device_id=dev, device_id_type=MESH)

    pl.when(r > 0)(lambda: hello(down))
    pl.when(r < R - 1)(lambda: hello(up))
    for o in range(1, C):
        hello({"col": (c + o) % C})
    hello(sib)
    for o in range(1, G):
        hello({"depth": (d + 2 * o) % Dp})
    peers = C + G - 1 + jnp.where(r > 0, 1, 0) + jnp.where(r < R - 1, 1, 0)
    pl.semaphore_wait(bar, peers)

    def ket_send(s, u, dirn, cond):
        send(kbuf.at[s, u], kbuf.at[s, u], ks_send.at[s, dirn, u], ks_recv.at[s, u],
             up if dirn else down, cond)

    for u in range(H):
        kloads[u].wait()
        ket_send(r, u, 0, r > 0)
        ket_send(r, u, 1, r < R - 1)
    loads[0].wait()
    loads[1].wait()
    for o in range(1, C):
        send(bbuf.at[c, h], bbuf.at[c, h], b_send.at[o], b_recv.at[0, c], {"col": (c + o) % C})
    loads[2].wait()

    for a in range(A):
        for b in range(B):
            keep = scr[b, a] > 0
            tile = traw[a, b]
            tmat[a * PS:(a + 1) * PS, b * PS:(b + 1) * PS] = jnp.where(keep, tile, jnp.zeros_like(tile))

    def ket_block(cb):
        x = bbuf[cb].reshape(rows, db)
        res = lax.dot_general(x, tmat[...], (((0,), (0,)), ((), ())), preferred_element_type=F32)
        for j in range(per):
            for u in range(H):
                kpart[cb * per + j, u] = res[j * dk:(j + 1) * dk, u * part:(u + 1) * part]

    def sum_send(t, u, dirn, cond):
        send(kpart.at[t, u], k_rx.at[dirn, t, u], kr_send.at[dirn, t, u], kr_recv.at[dirn, t, u],
             {"row": r - 1 + 2 * dirn}, cond)

    def sum_recv(t, u, dirn):
        recv(k_rx.at[dirn, t, u], kr_send.at[dirn, t, u], kr_recv.at[dirn, t, u])

    def ket_ends(cb):
        for j in range(per):
            t = cb * per + j
            for u in range(H):
                sum_send(t, u, 0, (r == R - 1) & (t < r))
        for j in reversed(range(per)):
            t = cb * per + j
            for u in range(H):
                sum_send(t, u, 1, (r == 0) & (t > r))

    first = (c * 2) // C

    def ket_forward(late, k):
        dirn = 1 - first if late else first
        t = jnp.where(dirn == 0, k, R - 1 - k)
        cond = jnp.where(dirn == 0, (r < R - 1) & (t < r), (r > 0) & (t > r))
        for u in range(H):
            def go():
                sum_recv(t, u, dirn)
                kpart[t, u] = kpart[t, u] + k_rx[dirn, t, u]
            pl.when(cond)(go)
            sum_send(t, u, dirn, cond)

    def ket_final():
        for u in range(H):
            at = slice(u * part, (u + 1) * part)
            out_k[:, at] = kpart[r, u]

            def take(dirn):
                sum_recv(r, u, dirn)
                out_k[:, at] += k_rx[dirn, r, u]
            pl.when(r < R - 1)(lambda: take(0))
            pl.when(r > 0)(lambda: take(1))

    near = jnp.minimum(r, R - 1 - r)

    def slot(i):
        k = (i + 1) // 2
        inner = r - k if i % 2 == 1 else r + k
        outer = jnp.where(r > R - 1 - r, r - (i - near), r + (i - near))
        return jnp.where(i <= 2 * near, inner, outer)

    order = [slot(i) for i in range(R)]

    def bra_a(i, close=None):
        s = order[i]
        here = None if close is None else (near >= 1 if close else near < 1)

        def gate(x):
            return x if here is None else x & here
        for u in range(H):
            recv(kbuf.at[s, u], ks_send.at[s, 0, u], ks_recv.at[s, u], here)
            ket_send(s, u, 0, gate((s > r) & (r > 0)))
            ket_send(s, u, 1, gate((s < r) & (r < R - 1)))

    def bra_dot(i):
        s = order[i]
        res = sum(
            lax.dot_general(kbuf[s, u], tmat[:, u * part:(u + 1) * part], (((1,), (1,)), ((), ())),
                            preferred_element_type=F32)
            for u in range(H))
        bp[s, 0] = res[:, :half]
        bp[s, 1] = res[:, half:]
        send(bp.at[s, 1 - h], d1_rx.at[s], bp_send.at[0, s], bp_recv.at[0, s], sib)

    def bra_b(i):
        s = order[i]
        cs, j = s // per, s % per
        recv(d1_rx.at[s], bp_send.at[0, s], bp_recv.at[0, s])
        bp[s, h] = bp[s, h] + d1_rx[s]
        send(bp.at[s, h], x_rx.at[c, j], bp_send.at[1, s], bp_recv.at[1, c * per + j], {"col": cs}, cs != c)

    def bra_c(i):
        s = order[i]
        cs, j = s // per, s % per

        def go():
            total = bp[s, h]
            for o in range(1, C):
                p = (c + o) % C
                recv(x_rx.at[p, j], bp_send.at[1, s], bp_recv.at[1, p * per + j])
                total = total + x_rx[p, j]
            y_rx[j, g] = total
        pl.when(cs == c)(go)
        for o in range(1, G):
            send(y_rx.at[j, g], y_rx.at[j, g], bp_send.at[1 + o, s], bp_recv.at[2, j * G + g],
                 {"depth": (d + 2 * o) % Dp}, cs == c)

    def bra_d(i):
        s = order[i]
        cs, j = s // per, s % per

        def go():
            for o in range(1, G):
                q = (g + o) % G
                recv(y_rx.at[j, q], bp_send.at[2, s], bp_recv.at[2, j * G + q])
            total = y_rx[j, 0]
            for q in range(1, G):
                total = total + y_rx[j, q]
            fin[j, h] = total
        pl.when(cs == c)(go)
        send(fin.at[j, h], fin.at[j, h], bp_send.at[G + 1, s], bp_recv.at[3, j], sib, cs == c)

    def bra_e():
        for j in range(per):
            recv(fin.at[j, 1 - h], bp_send.at[G + 1, 0], bp_recv.at[3, j])
            out_b[j * dk:(j + 1) * dk, :half] = fin[j, 0]
            out_b[j * dk:(j + 1) * dk, half:] = fin[j, 1]

    others = [(c + o) % C for o in range(1, C)]
    ket_block(c)
    ket_ends(c)
    bra_dot(0)
    bra_a(1)
    bra_b(0)
    bra_dot(1)
    for p in others:
        recv(bbuf.at[p, h], b_send.at[0], b_recv.at[0, p])
        send(bbuf.at[p, h], bbuf.at[p, h], b_send.at[C + p], b_recv.at[1, p], sib)
    bra_a(2, True)
    bra_b(1)
    for p in others:
        recv(bbuf.at[p, 1 - h], b_send.at[0], b_recv.at[1, p])
        ket_block(p)
        ket_ends(p)
    bra_a(2, False)
    bra_dot(2)
    bra_a(3, True)
    ket_forward(False, 0)
    bra_c(0)
    bra_b(2)
    bra_a(3, False)
    bra_dot(3)
    ket_forward(False, 1)
    bra_c(1)
    bra_b(3)
    for i in range(4, R):
        bra_a(i)
        bra_dot(i)
        bra_b(i)
    ket_forward(True, 0)
    bra_d(0)
    bra_c(2)
    for k in range(2, R - 1):
        ket_forward(False, k)
        ket_forward(True, k - 1)
    bra_d(1)
    bra_c(3)
    for i in range(4, R):
        bra_c(i)
    ket_forward(True, R - 2)
    for i in range(2, R):
        bra_d(i)
    bra_e()
    ket_final()

    for cond, wait in pending:
        if cond is None:
            wait()
        else:
            pl.when(cond)(wait)


def body(sizes, eri_tiles, screen, density_bra, density_ket):
    R, C, Dp = sizes
    A, B, PS, _ = eri_tiles.shape
    rows, cols = A * PS, B * PS
    db, dk = density_bra.shape[1], density_ket.shape[1]
    per, G, half, H = R // C, Dp // 2, rows // 2, 2
    DMA = pltpu.SemaphoreType.DMA
    anyspec = pl.BlockSpec(memory_space=pl.ANY)
    vm = pl.BlockSpec(memory_space=pltpu.VMEM)
    out_b, out_k = pl.pallas_call(
        functools.partial(kernel, sizes),
        out_shape=(jax.ShapeDtypeStruct((db, rows), F32), jax.ShapeDtypeStruct((dk, cols), F32)),
        in_specs=[anyspec, pl.BlockSpec(memory_space=pltpu.SMEM), anyspec, anyspec],
        out_specs=(vm, vm),
        scratch_shapes=[
            pltpu.VMEM((A, B, PS, PS), jnp.bfloat16),
            pltpu.VMEM((rows, cols), jnp.bfloat16),
            pltpu.VMEM((R, H, dk, cols // H), jnp.bfloat16),
            pltpu.VMEM((C, 2, half, db), jnp.bfloat16),
            pltpu.VMEM((R, H, dk, cols // H), F32),
            pltpu.VMEM((2, R, H, dk, cols // H), F32),
            pltpu.VMEM((R, 2, dk, half), F32),
            pltpu.VMEM((R, dk, half), F32),
            pltpu.VMEM((C, per, dk, half), F32),
            pltpu.VMEM((per, G, dk, half), F32),
            pltpu.VMEM((per, 2, dk, half), F32),
            DMA((3 + H,)),
            DMA((R, 2, H)), DMA((R, H)),
            DMA((2 * C,)), DMA((2, C)),
            DMA((2, R, H)), DMA((2, R, H)),
            DMA((G + 2, R)), DMA((4, max(R, per * G))),
        ],
        compiler_params=pltpu.CompilerParams(
            collective_id=0, has_side_effects=True, vmem_limit_bytes=28 * 1024 * 1024),
    )(eri_tiles, screen.T, density_bra, density_ket.T)
    return out_b.T, out_k.T


def solution(mesh):
    sizes = (mesh.shape["row"], mesh.shape["col"], mesh.shape["depth"])
    return jax.shard_map(
        functools.partial(body, sizes),
        mesh=mesh,
        in_specs=(
            P("row", ("col", "depth"), None, None),
            P("row", ("col", "depth")),
            P("row", "col"),
            P(("col", "depth"), "row"),
        ),
        out_specs=(P("row", "col"), P(("col", "depth"), "row")),
        check_vma=False,
    )
```

```python
import functools

import jax
import jax.numpy as jnp
from jax import lax
from jax.experimental import pallas as pl
from jax.experimental.pallas import tpu as pltpu
from jax.sharding import PartitionSpec as P

MESH = pl.DeviceIdType.MESH
F32 = jnp.float32


def kernel(
    sizes, eri, screen, dbra, dket, out_b, out_k,
    scr, traw, tmat, kbuf, bbuf, kpart, k_rx, bp, d1_rx, x_rx, y_rx, fin,
    local_sem, ks_send, ks_recv, b_send, b_recv, kr_send, kr_recv, bp_send, bp_recv,
):
    R, C, Dp = sizes
    per = R // C
    G = Dp // 2
    r, c, d = lax.axis_index("row"), lax.axis_index("col"), lax.axis_index("depth")
    h = d % 2
    g = d // 2
    sib = {"depth": d + 1 - 2 * h}
    up, down = {"row": r + 1}, {"row": r - 1}
    A, B, PS = eri.shape[0], eri.shape[1], eri.shape[2]
    rows, cols = tmat.shape
    dk = kbuf.shape[2]
    H = kbuf.shape[1]
    part = cols // H
    db = bbuf.shape[3]
    pending = []

    def send(src, dst, ssem, rsem, dev, cond=None):
        def make():
            return pltpu.make_async_remote_copy(
                src_ref=src, dst_ref=dst, send_sem=ssem, recv_sem=rsem,
                device_id=dev, device_id_type=MESH)

        def start():
            make().start()

        if cond is None:
            start()
        else:
            pl.when(cond)(start)
        pending.append((cond, lambda: make().wait_send()))

    def recv(dst, ssem, rsem, cond=None):
        def go():
            pltpu.make_async_remote_copy(
                src_ref=dst, dst_ref=dst, send_sem=ssem, recv_sem=rsem,
                device_id=sib, device_id_type=MESH).wait_recv()
        if cond is None:
            go()
        else:
            pl.when(cond)(go)

    half = rows // 2
    loads = [
        pltpu.make_async_copy(dbra.at[pl.ds(0, half)], bbuf.at[c, 0], local_sem.at[0]),
        pltpu.make_async_copy(dbra.at[pl.ds(half, half)], bbuf.at[c, 1], local_sem.at[1]),
        pltpu.make_async_copy(eri, traw, local_sem.at[2]),
        pltpu.make_async_copy(screen, scr, local_sem.at[3 + H]),
    ]
    kloads = [
        pltpu.make_async_copy(dket.at[:, pl.ds(u * part, part)], kbuf.at[r, u], local_sem.at[3 + u])
        for u in range(H)
    ]
    for one in kloads:
        one.start()
    for one in loads:
        one.start()

    bar = pltpu.get_barrier_semaphore()

    def hello(dev):
        pl.semaphore_signal(bar, inc=1, device_id=dev, device_id_type=MESH)

    pl.when(r > 0)(lambda: hello(down))
    pl.when(r < R - 1)(lambda: hello(up))
    for o in range(1, C):
        hello({"col": (c + o) % C})
    hello(sib)
    for o in range(1, G):
        hello({"depth": (d + 2 * o) % Dp})
    peers = C + G - 1 + jnp.where(r > 0, 1, 0) + jnp.where(r < R - 1, 1, 0)
    pl.semaphore_wait(bar, peers)

    def ket_send(s, u, dirn, cond):
        send(kbuf.at[s, u], kbuf.at[s, u], ks_send.at[s, dirn, u], ks_recv.at[s, u],
             up if dirn else down, cond)

    for u in range(H):
        kloads[u].wait()
        ket_send(r, u, 0, r > 0)
        ket_send(r, u, 1, r < R - 1)
    loads[0].wait()
    loads[1].wait()
    for o in range(1, C):
        send(bbuf.at[c, h], bbuf.at[c, h], b_send.at[o], b_recv.at[0, c], {"col": (c + o) % C})
    loads[2].wait()
    loads[3].wait()

    for a in range(A):
        for b in range(B):
            keep = scr[b, a] > 0
            tile = traw[a, b]
            tmat[a * PS:(a + 1) * PS, b * PS:(b + 1) * PS] = jnp.where(keep, tile, jnp.zeros_like(tile))

    def ket_block(cb):
        x = bbuf[cb].reshape(rows, db)
        res = lax.dot_general(x, tmat[...], (((0,), (0,)), ((), ())), preferred_element_type=F32)
        for j in range(per):
            for u in range(H):
                kpart[cb * per + j, u] = res[j * dk:(j + 1) * dk, u * part:(u + 1) * part]

    def sum_send(t, u, dirn, cond):
        send(kpart.at[t, u], k_rx.at[dirn, t, u], kr_send.at[dirn, t, u], kr_recv.at[dirn, t, u],
             {"row": r - 1 + 2 * dirn}, cond)

    def sum_recv(t, u, dirn):
        recv(k_rx.at[dirn, t, u], kr_send.at[dirn, t, u], kr_recv.at[dirn, t, u])

    def ket_ends(cb):
        for j in range(per):
            t = cb * per + j
            for u in range(H):
                sum_send(t, u, 0, (r == R - 1) & (t < r))
        for j in reversed(range(per)):
            t = cb * per + j
            for u in range(H):
                sum_send(t, u, 1, (r == 0) & (t > r))

    first = (c * 2) // C

    def ket_forward(late, k):
        dirn = 1 - first if late else first
        t = jnp.where(dirn == 0, k, R - 1 - k)
        cond = jnp.where(dirn == 0, (r < R - 1) & (t < r), (r > 0) & (t > r))
        for u in range(H):
            def go():
                sum_recv(t, u, dirn)
                kpart[t, u] = kpart[t, u] + k_rx[dirn, t, u]
            pl.when(cond)(go)
            sum_send(t, u, dirn, cond)

    def ket_final():
        for u in range(H):
            at = slice(u * part, (u + 1) * part)
            out_k[:, at] = kpart[r, u]

            def take(dirn):
                sum_recv(r, u, dirn)
                out_k[:, at] += k_rx[dirn, r, u]
            pl.when(r < R - 1)(lambda: take(0))
            pl.when(r > 0)(lambda: take(1))

    near = jnp.minimum(r, R - 1 - r)

    def slot(i):
        k = (i + 1) // 2
        inner = r - k if i % 2 == 1 else r + k
        outer = jnp.where(r > R - 1 - r, r - (i - near), r + (i - near))
        return jnp.where(i <= 2 * near, inner, outer)

    order = [slot(i) for i in range(R)]

    def bra_a(i, close=None):
        s = order[i]
        here = None if close is None else (near >= 1 if close else near < 1)

        def gate(x):
            return x if here is None else x & here
        for u in range(H):
            recv(kbuf.at[s, u], ks_send.at[s, 0, u], ks_recv.at[s, u], here)
            ket_send(s, u, 0, gate((s > r) & (r > 0)))
            ket_send(s, u, 1, gate((s < r) & (r < R - 1)))

    def bra_dot(i):
        s = order[i]
        res = sum(
            lax.dot_general(kbuf[s, u], tmat[:, u * part:(u + 1) * part], (((1,), (1,)), ((), ())),
                            preferred_element_type=F32)
            for u in range(H))
        bp[s, 0] = res[:, :half]
        bp[s, 1] = res[:, half:]
        send(bp.at[s, 1 - h], d1_rx.at[s], bp_send.at[0, s], bp_recv.at[0, s], sib)

    def bra_b(i):
        s = order[i]
        cs, j = s // per, s % per
        recv(d1_rx.at[s], bp_send.at[0, s], bp_recv.at[0, s])
        bp[s, h] = bp[s, h] + d1_rx[s]
        send(bp.at[s, h], x_rx.at[c, j], bp_send.at[1, s], bp_recv.at[1, c * per + j], {"col": cs}, cs != c)

    def bra_c(i):
        s = order[i]
        cs, j = s // per, s % per

        def go():
            total = bp[s, h]
            for o in range(1, C):
                p = (c + o) % C
                recv(x_rx.at[p, j], bp_send.at[1, s], bp_recv.at[1, p * per + j])
                total = total + x_rx[p, j]
            y_rx[j, g] = total
        pl.when(cs == c)(go)
        for o in range(1, G):
            send(y_rx.at[j, g], y_rx.at[j, g], bp_send.at[1 + o, s], bp_recv.at[2, j * G + g],
                 {"depth": (d + 2 * o) % Dp}, cs == c)

    def bra_d(i):
        s = order[i]
        cs, j = s // per, s % per

        def go():
            for o in range(1, G):
                q = (g + o) % G
                recv(y_rx.at[j, q], bp_send.at[2, s], bp_recv.at[2, j * G + q])
            total = y_rx[j, 0]
            for q in range(1, G):
                total = total + y_rx[j, q]
            fin[j, h] = total
        pl.when(cs == c)(go)
        send(fin.at[j, h], fin.at[j, h], bp_send.at[G + 1, s], bp_recv.at[3, j], sib, cs == c)

    def bra_e():
        for j in range(per):
            recv(fin.at[j, 1 - h], bp_send.at[G + 1, 0], bp_recv.at[3, j])
            out_b[j * dk:(j + 1) * dk, :half] = fin[j, 0]
            out_b[j * dk:(j + 1) * dk, half:] = fin[j, 1]

    others = [(c + o) % C for o in range(1, C)]
    ket_block(c)
    ket_ends(c)
    bra_dot(0)
    bra_a(1)
    bra_b(0)
    bra_dot(1)
    for p in others:
        recv(bbuf.at[p, h], b_send.at[0], b_recv.at[0, p])
        send(bbuf.at[p, h], bbuf.at[p, h], b_send.at[C + p], b_recv.at[1, p], sib)
    bra_a(2, True)
    bra_b(1)
    for p in others:
        recv(bbuf.at[p, 1 - h], b_send.at[0], b_recv.at[1, p])
        ket_block(p)
        ket_ends(p)
    bra_a(2, False)
    bra_dot(2)
    bra_a(3, True)
    ket_forward(False, 0)
    bra_c(0)
    bra_b(2)
    bra_a(3, False)
    bra_dot(3)
    ket_forward(False, 1)
    bra_c(1)
    bra_b(3)
    for i in range(4, R):
        bra_a(i)
        bra_dot(i)
        bra_b(i)
    ket_forward(True, 0)
    bra_d(0)
    bra_c(2)
    for k in range(2, R - 1):
        ket_forward(False, k)
        ket_forward(True, k - 1)
    bra_d(1)
    bra_c(3)
    for i in range(4, R):
        bra_c(i)
    ket_forward(True, R - 2)
    for i in range(2, R):
        bra_d(i)
    bra_e()
    ket_final()

    for cond, wait in pending:
        if cond is None:
            wait()
        else:
            pl.when(cond)(wait)


def body(sizes, eri_tiles, screen, density_bra, density_ket):
    R, C, Dp = sizes
    A, B, PS, _ = eri_tiles.shape
    rows, cols = A * PS, B * PS
    db, dk = density_bra.shape[1], density_ket.shape[1]
    per, G, half, H = R // C, Dp // 2, rows // 2, 2
    DMA = pltpu.SemaphoreType.DMA
    hbm = pl.BlockSpec(memory_space=pltpu.HBM)
    vm = pl.BlockSpec(memory_space=pltpu.VMEM)
    out_b, out_k = pl.pallas_call(
        functools.partial(kernel, sizes),
        out_shape=(jax.ShapeDtypeStruct((db, rows), F32), jax.ShapeDtypeStruct((dk, cols), F32)),
        in_specs=[hbm, hbm, hbm, hbm],
        out_specs=(vm, vm),
        scratch_shapes=[
            pltpu.SMEM((B, A), jnp.int32),
            pltpu.VMEM((A, B, PS, PS), jnp.bfloat16),
            pltpu.VMEM((rows, cols), jnp.bfloat16),
            pltpu.VMEM((R, H, dk, cols // H), jnp.bfloat16),
            pltpu.VMEM((C, 2, half, db), jnp.bfloat16),
            pltpu.VMEM((R, H, dk, cols // H), F32),
            pltpu.VMEM((2, R, H, dk, cols // H), F32),
            pltpu.VMEM((R, 2, dk, half), F32),
            pltpu.VMEM((R, dk, half), F32),
            pltpu.VMEM((C, per, dk, half), F32),
            pltpu.VMEM((per, G, dk, half), F32),
            pltpu.VMEM((per, 2, dk, half), F32),
            DMA((4 + H,)),
            DMA((R, 2, H)), DMA((R, H)),
            DMA((2 * C,)), DMA((2, C)),
            DMA((2, R, H)), DMA((2, R, H)),
            DMA((G + 2, R)), DMA((4, max(R, per * G))),
        ],
        compiler_params=pltpu.CompilerParams(
            collective_id=0, has_side_effects=True, vmem_limit_bytes=28 * 1024 * 1024),
    )(*(pltpu.with_memory_space_constraint(x, pltpu.HBM) for x in (eri_tiles, screen.T, density_bra, density_ket.T)))
    return out_b.T, out_k.T


def solution(mesh):
    sizes = (mesh.shape["row"], mesh.shape["col"], mesh.shape["depth"])
    return jax.shard_map(
        functools.partial(body, sizes),
        mesh=mesh,
        in_specs=(
            P("row", ("col", "depth"), None, None),
            P("row", ("col", "depth")),
            P("row", "col"),
            P(("col", "depth"), "row"),
        ),
        out_specs=(P("row", "col"), P(("col", "depth"), "row")),
        check_vma=False,
    )
```

```python
import functools

import jax
import jax.numpy as jnp
from jax import lax
from jax.experimental import pallas as pl
from jax.experimental.pallas import tpu as pltpu
from jax.sharding import PartitionSpec as P

MESH = pl.DeviceIdType.MESH
F32 = jnp.float32


def kernel(
    sizes, eri, screen, dbra, dket, out_b, out_k,
    scr, traw, tmat, kbuf, bbuf, kpart, k_rx, bp, d1_rx, x_rx, y_rx, fin,
    local_sem, ks_send, ks_recv, b_send, b_recv, kr_send, kr_recv, bp_send, bp_recv,
):
    R, C, Dp = sizes
    per = R // C
    G = Dp // 2
    r, c, d = lax.axis_index("row"), lax.axis_index("col"), lax.axis_index("depth")
    h = d % 2
    g = d // 2
    sib = {"depth": d + 1 - 2 * h}
    up, down = {"row": r + 1}, {"row": r - 1}
    A, B, PS = eri.shape[0], eri.shape[1], eri.shape[2]
    rows, cols = tmat.shape
    dk = kbuf.shape[2]
    H = kbuf.shape[1]
    part = cols // H
    db = bbuf.shape[3]
    pending = []

    def send(src, dst, ssem, rsem, dev, cond=None):
        def make():
            return pltpu.make_async_remote_copy(
                src_ref=src, dst_ref=dst, send_sem=ssem, recv_sem=rsem,
                device_id=dev, device_id_type=MESH)

        def start():
            make().start()

        if cond is None:
            start()
        else:
            pl.when(cond)(start)
        pending.append((cond, lambda: make().wait_send()))

    def recv(dst, ssem, rsem, cond=None):
        def go():
            pltpu.make_async_remote_copy(
                src_ref=dst, dst_ref=dst, send_sem=ssem, recv_sem=rsem,
                device_id=sib, device_id_type=MESH).wait_recv()
        if cond is None:
            go()
        else:
            pl.when(cond)(go)

    half = rows // 2
    loads = [
        pltpu.make_async_copy(dbra.at[pl.ds(0, half)], bbuf.at[c, 0], local_sem.at[0]),
        pltpu.make_async_copy(dbra.at[pl.ds(half, half)], bbuf.at[c, 1], local_sem.at[1]),
        pltpu.make_async_copy(eri, traw, local_sem.at[2]),
        pltpu.make_async_copy(screen, scr, local_sem.at[3 + H]),
    ]
    kloads = [
        pltpu.make_async_copy(dket.at[:, pl.ds(u * part, part)], kbuf.at[r, u], local_sem.at[3 + u])
        for u in range(H)
    ]
    for one in kloads:
        one.start()
    for one in loads:
        one.start()

    bar = pltpu.get_barrier_semaphore()

    def hello(dev):
        pl.semaphore_signal(bar, inc=1, device_id=dev, device_id_type=MESH)

    pl.when(r > 0)(lambda: hello(down))
    pl.when(r < R - 1)(lambda: hello(up))
    for o in range(1, C):
        hello({"col": (c + o) % C})
    hello(sib)
    for o in range(1, G):
        hello({"depth": (d + 2 * o) % Dp})
    peers = C + G - 1 + jnp.where(r > 0, 1, 0) + jnp.where(r < R - 1, 1, 0)
    pl.semaphore_wait(bar, peers)

    def ket_send(s, u, dirn, cond):
        send(kbuf.at[s, u], kbuf.at[s, u], ks_send.at[s, dirn, u], ks_recv.at[s, u],
             up if dirn else down, cond)

    for u in range(H):
        kloads[u].wait()
        ket_send(r, u, 0, r > 0)
        ket_send(r, u, 1, r < R - 1)
    loads[0].wait()
    loads[1].wait()
    for o in range(1, C):
        send(bbuf.at[c, h], bbuf.at[c, h], b_send.at[o], b_recv.at[0, c], {"col": (c + o) % C})
    loads[2].wait()
    loads[3].wait()

    for a in range(A):
        for b in range(B):
            keep = scr[b, a] > 0
            tile = traw[a, b]
            tmat[a * PS:(a + 1) * PS, b * PS:(b + 1) * PS] = jnp.where(keep, tile, jnp.zeros_like(tile))

    def ket_block(cb):
        x = bbuf[cb].reshape(rows, db)
        res = lax.dot_general(x, tmat[...], (((0,), (0,)), ((), ())), preferred_element_type=F32)
        for j in range(per):
            for u in range(H):
                kpart[cb * per + j, u] = res[j * dk:(j + 1) * dk, u * part:(u + 1) * part]

    def sum_send(t, u, dirn, cond):
        send(kpart.at[t, u], k_rx.at[dirn, t, u], kr_send.at[dirn, t, u], kr_recv.at[dirn, t, u],
             {"row": r - 1 + 2 * dirn}, cond)

    def sum_recv(t, u, dirn):
        recv(k_rx.at[dirn, t, u], kr_send.at[dirn, t, u], kr_recv.at[dirn, t, u])

    def ket_ends(cb):
        for j in range(per):
            t = cb * per + j
            for u in range(H):
                sum_send(t, u, 0, (r == R - 1) & (t < r))
        for j in reversed(range(per)):
            t = cb * per + j
            for u in range(H):
                sum_send(t, u, 1, (r == 0) & (t > r))

    first = (c * 2) // C

    def ket_forward(late, k):
        dirn = 1 - first if late else first
        t = jnp.where(dirn == 0, k, R - 1 - k)
        cond = jnp.where(dirn == 0, (r < R - 1) & (t < r), (r > 0) & (t > r))
        for u in range(H):
            def go():
                sum_recv(t, u, dirn)
                kpart[t, u] = kpart[t, u] + k_rx[dirn, t, u]
            pl.when(cond)(go)
            sum_send(t, u, dirn, cond)

    def ket_final():
        for u in range(H):
            at = slice(u * part, (u + 1) * part)
            out_k[:, at] = kpart[r, u]

            def take(dirn):
                sum_recv(r, u, dirn)
                out_k[:, at] += k_rx[dirn, r, u]
            pl.when(r < R - 1)(lambda: take(0))
            pl.when(r > 0)(lambda: take(1))

    near = jnp.minimum(r, R - 1 - r)

    def slot(i):
        k = (i + 1) // 2
        inner = r - k if i % 2 == 1 else r + k
        outer = jnp.where(r > R - 1 - r, r - (i - near), r + (i - near))
        return jnp.where(i <= 2 * near, inner, outer)

    order = [slot(i) for i in range(R)]

    def bra_a(i, close=None):
        s = order[i]
        here = None if close is None else (near >= 1 if close else near < 1)

        def gate(x):
            return x if here is None else x & here
        for u in range(H):
            recv(kbuf.at[s, u], ks_send.at[s, 0, u], ks_recv.at[s, u], here)
            ket_send(s, u, 0, gate((s > r) & (r > 0)))
            ket_send(s, u, 1, gate((s < r) & (r < R - 1)))

    def bra_dot(i):
        s = order[i]
        res = sum(
            lax.dot_general(kbuf[s, u], tmat[:, u * part:(u + 1) * part], (((1,), (1,)), ((), ())),
                            preferred_element_type=F32)
            for u in range(H))
        bp[s, 0] = res[:, :half]
        bp[s, 1] = res[:, half:]
        send(bp.at[s, 1 - h], d1_rx.at[s], bp_send.at[0, s], bp_recv.at[0, s], sib)

    def bra_b(i):
        s = order[i]
        cs, j = s // per, s % per
        recv(d1_rx.at[s], bp_send.at[0, s], bp_recv.at[0, s])
        bp[s, h] = bp[s, h] + d1_rx[s]
        send(bp.at[s, h], x_rx.at[c, j], bp_send.at[1, s], bp_recv.at[1, c * per + j], {"col": cs}, cs != c)

    def bra_c(i):
        s = order[i]
        cs, j = s // per, s % per

        def go():
            total = bp[s, h]
            for o in range(1, C):
                p = (c + o) % C
                recv(x_rx.at[p, j], bp_send.at[1, s], bp_recv.at[1, p * per + j])
                total = total + x_rx[p, j]
            y_rx[j, g] = total
        pl.when(cs == c)(go)
        for o in range(1, G):
            send(y_rx.at[j, g], y_rx.at[j, g], bp_send.at[1 + o, s], bp_recv.at[2, j * G + g],
                 {"depth": (d + 2 * o) % Dp}, cs == c)

    def bra_d(i):
        s = order[i]
        cs, j = s // per, s % per

        def go():
            for o in range(1, G):
                q = (g + o) % G
                recv(y_rx.at[j, q], bp_send.at[2, s], bp_recv.at[2, j * G + q])
            total = y_rx[j, 0]
            for q in range(1, G):
                total = total + y_rx[j, q]
            fin[j, h] = total
        pl.when(cs == c)(go)
        send(fin.at[j, h], fin.at[j, h], bp_send.at[G + 1, s], bp_recv.at[3, j], sib, cs == c)

    def bra_e():
        for j in range(per):
            recv(fin.at[j, 1 - h], bp_send.at[G + 1, 0], bp_recv.at[3, j])
            out_b[j * dk:(j + 1) * dk, :half] = fin[j, 0]
            out_b[j * dk:(j + 1) * dk, half:] = fin[j, 1]

    others = [(c + o) % C for o in range(1, C)]
    ket_block(c)
    ket_ends(c)
    bra_dot(0)
    bra_a(1)
    bra_b(0)
    bra_dot(1)
    for p in others:
        recv(bbuf.at[p, h], b_send.at[0], b_recv.at[0, p])
        send(bbuf.at[p, h], bbuf.at[p, h], b_send.at[C + p], b_recv.at[1, p], sib)
    bra_a(2, True)
    bra_b(1)
    for p in others:
        recv(bbuf.at[p, 1 - h], b_send.at[0], b_recv.at[1, p])
        ket_block(p)
        ket_ends(p)
    bra_a(2, False)
    bra_dot(2)
    bra_a(3, True)
    ket_forward(False, 0)
    bra_c(0)
    bra_b(2)
    bra_a(3, False)
    bra_dot(3)
    ket_forward(False, 1)
    bra_c(1)
    bra_b(3)
    for i in range(4, R):
        bra_a(i)
        bra_dot(i)
        bra_b(i)
    bra_c(2)
    ket_forward(True, 0)
    bra_c(3)
    bra_d(0)
    for k in range(2, R - 1):
        ket_forward(False, k)
        ket_forward(True, k - 1)
    bra_d(1)
    for i in range(4, R):
        bra_c(i)
    ket_forward(True, R - 2)
    for i in range(2, R):
        bra_d(i)
    bra_e()
    ket_final()

    for cond, wait in pending:
        if cond is None:
            wait()
        else:
            pl.when(cond)(wait)


def body(sizes, eri_tiles, screen, density_bra, density_ket):
    R, C, Dp = sizes
    A, B, PS, _ = eri_tiles.shape
    rows, cols = A * PS, B * PS
    db, dk = density_bra.shape[1], density_ket.shape[1]
    per, G, half, H = R // C, Dp // 2, rows // 2, 2
    DMA = pltpu.SemaphoreType.DMA
    hbm = pl.BlockSpec(memory_space=pltpu.HBM)
    vm = pl.BlockSpec(memory_space=pltpu.VMEM)
    out_b, out_k = pl.pallas_call(
        functools.partial(kernel, sizes),
        out_shape=(jax.ShapeDtypeStruct((db, rows), F32), jax.ShapeDtypeStruct((dk, cols), F32)),
        in_specs=[hbm, hbm, hbm, hbm],
        out_specs=(vm, vm),
        scratch_shapes=[
            pltpu.SMEM((B, A), jnp.int32),
            pltpu.VMEM((A, B, PS, PS), jnp.bfloat16),
            pltpu.VMEM((rows, cols), jnp.bfloat16),
            pltpu.VMEM((R, H, dk, cols // H), jnp.bfloat16),
            pltpu.VMEM((C, 2, half, db), jnp.bfloat16),
            pltpu.VMEM((R, H, dk, cols // H), F32),
            pltpu.VMEM((2, R, H, dk, cols // H), F32),
            pltpu.VMEM((R, 2, dk, half), F32),
            pltpu.VMEM((R, dk, half), F32),
            pltpu.VMEM((C, per, dk, half), F32),
            pltpu.VMEM((per, G, dk, half), F32),
            pltpu.VMEM((per, 2, dk, half), F32),
            DMA((4 + H,)),
            DMA((R, 2, H)), DMA((R, H)),
            DMA((2 * C,)), DMA((2, C)),
            DMA((2, R, H)), DMA((2, R, H)),
            DMA((G + 2, R)), DMA((4, max(R, per * G))),
        ],
        compiler_params=pltpu.CompilerParams(
            collective_id=0, has_side_effects=True, vmem_limit_bytes=28 * 1024 * 1024),
    )(*(pltpu.with_memory_space_constraint(x, pltpu.HBM) for x in (eri_tiles, screen.T, density_bra, density_ket.T)))
    return out_b.T, out_k.T


def solution(mesh):
    sizes = (mesh.shape["row"], mesh.shape["col"], mesh.shape["depth"])
    return jax.shard_map(
        functools.partial(body, sizes),
        mesh=mesh,
        in_specs=(
            P("row", ("col", "depth"), None, None),
            P("row", ("col", "depth")),
            P("row", "col"),
            P(("col", "depth"), "row"),
        ),
        out_specs=(P("row", "col"), P(("col", "depth"), "row")),
        check_vma=False,
    )
```
